32 devices in a mesh: grp: 2 (over x), layer: 4 (over z), feat: 4 (over y, core).
Axes of the slice: x: 2, y: 2, z: 4, core: 2. Of those that a mesh axis runs over, the one named last changes fastest.
Arguments:
- inputs: bfloat16 [4, 512, 2304], P('layer', ('grp', 'feat')), may hold values from -6 to 6
- targets: bfloat16 [512, 4, 2304], P(('grp', 'feat'), None, 'layer'), may hold values from -6 to 6
- enc_weight: bfloat16 [4, 2304, 8192], P('layer', None, 'feat'), may hold values from -0.125 to 0.125
- enc_bias: float32 [4, 8192], P('layer', 'feat'), may hold values from -3 to 3
- dec_weight: bfloat16 [10, 8192, 2304], P(None, 'feat', 'layer'), may hold values from -0.0625 to 0.0625
- dec_bias: float32 [4, 2304], P(None, 'layer'), may hold values from -3 to 3
Outputs:
- enc_grad: bfloat16 [4, 2304, 8192], P('layer', 'grp', 'feat')
- enc_bias_grad: float32 [4, 8192], P('layer', 'feat')
- dec_grad: bfloat16 [10, 8192, 2304], P('grp', 'feat', 'layer')
- dec_bias_grad: float32 [4, 2304], P(None, 'layer')
The draws below stay inside these ranges and needn't reach their ends.
All inputs are finite; a program needn't handle non-finite values.
Results may differ from the reference program's by a relative error of at most 0.019.
Values may be sent and summed in bfloat16 or wider, within the bound.
A program may use at most 128 MiB of HBM per device.

```python
import jax
import jax.numpy as jnp

D = 2304
FEATS = 8192
LAYERS = 4
PAIRS = 10
TOKENS = 512


def block_scale(own_key, shape, pieces, least, top_value):
    level = 1.0
    for axis_at, parts in pieces:
        steps = jax.random.uniform(jax.random.fold_in(jax.random.fold_in(own_key, 6), axis_at), (parts,), jnp.float32, least / len(pieces), top_value / len(pieces))
        level = level * jnp.repeat(jnp.exp(steps), shape[axis_at] // parts).reshape((-1,) + (1,) * (len(shape) - 1 - axis_at))
    return level


def gaussian(rng, dims, deviation, bound, cuts=(), held_as=jnp.bfloat16):
    values = jax.random.normal(rng, dims, jnp.float32) * deviation
    if len(cuts) > 0:
        values = block_scale(rng, dims, cuts, -0.22, 0.18) * values
    return jnp.clip(values, min=-bound, max=bound).astype(held_as)


def setup_inputs(seed: int = 0) -> dict:
    streams_of = jax.random.split(jax.random.key(seed), 7)
    inputs = gaussian(streams_of[0], (LAYERS, TOKENS, D), 1.0, 6.0, ((0, 4), (1, 8)))
    targets = gaussian(streams_of[1], (TOKENS, LAYERS, D), 1.0, 6.0, ((0, 8), (2, 4)))
    enc_weight = gaussian(streams_of[2], (LAYERS, D, FEATS), D ** -0.5, 0.125, ((0, 4), (2, 4)))
    enc_bias = gaussian(streams_of[3], (LAYERS, FEATS), 0.5, 3.0, ((0, 4), (1, 4)), jnp.float32)
    dec_weight = gaussian(streams_of[4], (PAIRS, FEATS, D), FEATS ** -0.5, 0.0625, ((1, 4), (2, 4)))
    dec_bias = gaussian(streams_of[5], (LAYERS, D), 0.5, 3.0, ((1, 4),), jnp.float32)
    return dict(inputs=inputs, targets=targets, enc_weight=enc_weight, enc_bias=enc_bias, dec_weight=dec_weight, dec_bias=dec_bias)


def pair_list(count):
    return [(source, target) for source in range(count) for target in range(source, count)]


def reference(inputs, targets, enc_weight, enc_bias, dec_weight, dec_bias):
    pairs = pair_list(LAYERS)
    pre = [jnp.dot(inputs[s], enc_weight[s], preferred_element_type=jnp.float32) + enc_bias[s] for s in range(LAYERS)]
    acts = [jnp.maximum(value, 0.0).astype(jnp.bfloat16) for value in pre]
    errors = []
    for target in range(LAYERS):
        total = jnp.zeros((TOKENS, D), jnp.float32) + dec_bias[target].astype(jnp.float32)
        for index, (source, later) in enumerate(pairs):
            if later == target:
                total = total + jnp.dot(acts[source], dec_weight[index], preferred_element_type=jnp.float32)
        errors.append(total - targets[:, target, :].astype(jnp.float32))
    dec_bias_grad = jnp.stack([jnp.sum(value, axis=0) for value in errors]) / TOKENS
    derr = [(value / TOKENS).astype(jnp.bfloat16) for value in errors]
    dec_grad = jnp.stack([jnp.dot(acts[s].T, derr[t], preferred_element_type=jnp.float32) for (s, t) in pairs]).astype(jnp.bfloat16)
    enc_grads = []
    bias_grads = []
    for source in range(LAYERS):
        dacts = jnp.zeros((TOKENS, FEATS), jnp.float32)
        for index, (first, target) in enumerate(pairs):
            if first == source:
                dacts = dacts + jnp.dot(derr[target], dec_weight[index].T, preferred_element_type=jnp.float32)
        dpre = jnp.where(pre[source] > 0, dacts, jnp.zeros_like(dacts))
        bias_grads.append(jnp.sum(dpre, axis=0))
        enc_grads.append(jnp.dot(inputs[source].T, dpre.astype(jnp.bfloat16), preferred_element_type=jnp.float32).astype(jnp.bfloat16))
    return jnp.stack(enc_grads), jnp.stack(bias_grads), dec_grad, dec_bias_grad
```

```python
import functools

import jax
import jax.numpy as jnp
from jax import lax
from jax.experimental import pallas as pl
from jax.experimental.pallas import tpu as pltpu
from jax.sharding import PartitionSpec as P

MESH = pl.DeviceIdType.MESH
BF = jnp.bfloat16
F32 = jnp.float32


def pair_list(count):
    return [(source, target) for source in range(count) for target in range(source, count)]


CHUNKS = 2


def dot_nn(a, b):
    return lax.dot_general(a, b, (((1,), (0,)), ((), ())), preferred_element_type=F32)


def dot_nt(a, b):
    return lax.dot_general(a, b, (((1,), (1,)), ((), ())), preferred_element_type=F32)


def dot_tn(a, b):
    return lax.dot_general(a, b, (((0,), (0,)), ((), ())), preferred_element_type=F32)


def rdma(src, dst, ssem, rsem, dev):
    return pltpu.make_async_remote_copy(
        src_ref=src, dst_ref=dst, send_sem=ssem, recv_sem=rsem, device_id=dev, device_id_type=MESH
    )


def kernel(cfg, *refs):
    (L, F, C, B, D, feats, width, cw, per, total, ranges, turned) = cfg
    if not turned:
        refs = refs[:18] + (None,) + refs[18:]
    (inp, tgt, ew, eb, dw, db, eg_o, ebg_o, dg_o, dbg_o,
     w_v, ew_v, acts, rows_v, cols_o, cols_t, acc, derr, derr_t,
     r1b, r1r, r2r, dpre, og_v, eg_v, dbs, dbr, dbx, ebs, ebr,
     ld_w, ld_ew, ld_in, in_p, in_s, in_r, co, zr_s, zl_s, z_r, x_s, x_r, r1_s, r1_r, r2_s, r2_r,
     ag_p, ag_s, ag_r, dx_s, dx_r, db_s, db_r, dbx_m, eb_m, b_s, b_r, dp_s, dp_r, og_m, eg_m) = refs
    g = lax.axis_index("grp")
    l = lax.axis_index("layer")
    f = lax.axis_index("feat")
    Q = feats // cw
    R = F * B
    n = C * R
    H = F // 2
    half = D // 2
    core = lax.rem(f, 2)
    chip = f // 2
    sib = f + 1 - 2 * core
    other = 1 - g
    xdev, sdev = (other, l, f), (g, l, sib)
    rdev, ldev = (g, l + 1, f), (g, l - 1, f)
    has_l, has_r = l > 0, l < L - 1

    def peer(k):
        j = lax.rem(chip + k, H)
        return j, 2 * j + core

    def by_group(which, values):
        return jnp.where(which == 0, values[0], values[1])

    def pair(s, t):
        return s * L - (s * (s - 1)) // 2 + t - s

    def brow(idx, n):
        return pl.ds(pl.multiple_of(idx * n, n), n)

    def need_s(h, s):
        return jnp.logical_and(s >= by_group(h, ranges[0]), s <= by_group(h, ranges[1]))

    def need_t(h, t):
        return jnp.logical_and(t >= by_group(h, ranges[2]), t <= by_group(h, ranges[3]))

    lin = [pltpu.make_async_copy(inp.at[0, pl.ds(c * B, B), :], rows_v.at[brow(c * F + f, B), :], ld_in.at[c])
           for c in range(C)]
    for cp in lin:
        cp.start()
    lew = [pltpu.make_async_copy(ew.at[0, :, pl.ds(q * cw, cw)], ew_v.at[q, pl.ds(0, D), :], ld_ew.at[q])
           for q in range(Q)]
    for cp in lew:
        cp.start()
    lw = [pltpu.make_async_copy(dw.at[p], w_v.at[p], ld_w.at[p]) for p in range(2 * per)]
    for cp in lw:
        cp.start()

    bar = pltpu.get_barrier_semaphore()
    pl.semaphore_signal(bar, inc=1, device_id=xdev, device_id_type=MESH)
    for k in range(1, F):
        pl.semaphore_signal(bar, inc=1, device_id=(g, l, lax.rem(f + k, F)), device_id_type=MESH)

    @pl.when(has_l)
    def _():
        pl.semaphore_signal(bar, inc=1, device_id=ldev, device_id_type=MESH)

    @pl.when(has_r)
    def _():
        pl.semaphore_signal(bar, inc=1, device_id=rdev, device_id_type=MESH)

    pl.semaphore_wait(bar, F + has_l.astype(jnp.int32) + has_r.astype(jnp.int32))

    def row_block(c, owner):
        return rows_v.at[brow(c * F + owner, B), :]

    for c in range(C):
        lin[c].wait()
        mine = row_block(c, f)
        for k in range(1, H):
            _, dev = peer(k)
            rdma(mine, mine, in_p.at[c, k], in_r.at[c, f], (g, l, dev)).start()
        rdma(mine, mine, in_s.at[c, f], in_r.at[c, f], sdev).start()
    acc[...] = jnp.zeros_like(acc)
    dbs[...] = jnp.zeros_like(dbs)
    ebs[...] = jnp.zeros_like(ebs)
    for c in range(C):
        for k in range(1, H):
            _, dev = peer(k)
            blk = row_block(c, dev)
            rdma(blk, blk, in_p.at[c, k], in_r.at[c, dev], sdev).wait_recv()
            rdma(blk, blk, in_s.at[c, dev], in_r.at[c, dev], sdev).start()
        for j in range(H):
            own = 2 * j + 1 - core
            blk = row_block(c, own)
            rdma(blk, blk, in_s.at[c, own], in_r.at[c, own], sdev).wait_recv()

    def cols_copy():
        cols = pl.ds(pl.multiple_of(other * half, half), half)
        return rdma(rows_v.at[:, cols], cols_o, co.at[0], co.at[1], xdev)

    cols_copy().start()

    def act_ref(c, s, q):
        return acts.at[s, q, pl.ds(c * R, R), :]

    def z_right(c, s, q):
        blk = act_ref(c, s, q)
        return rdma(blk, blk, zr_s.at[c, s, q], z_r.at[c, s, q], rdev)

    def z_left(c, s, q):
        blk = act_ref(c, s, q)
        return rdma(blk, blk, zl_s.at[c, s, q], z_r.at[c, s, q], ldev)

    def x_copy(c, s, q):
        return rdma(act_ref(c, s, q), acts.at[s, q, pl.ds(n + c * R, R), :], x_s.at[c, s, q], x_r.at[c, s, q], xdev)

    def decode(c, s, q):
        def one(t, carry):
            acc[c, t] += dot_nt(act_ref(c, s, q)[...], w_v[pair(s, t), :, brow(q, cw)])
            return carry

        lax.fori_loop(s, L, one, 0)

    def encode(q, carry):
        pltpu.make_async_copy(
            ew.at[0, :, pl.ds(pl.multiple_of(q * cw, cw), cw)], ew_v.at[q, pl.ds(0, D), :], ld_ew.at[q]
        ).wait()
        bias = eb[:, pl.ds(pl.multiple_of(q * cw, cw), cw)]
        pre = dot_nn(rows_v[...], ew_v[q, pl.ds(0, D), :]) + bias
        acts[l, q, pl.ds(0, n), :] = jnp.maximum(pre, 0.0).astype(BF)
        send_own(0, q)
        return carry

    def send_own(c, q):
        @pl.when(has_r)
        def _():
            z_right(c, l, q).start()

        @pl.when(has_l)
        def _():
            z_left(c, l, q).start()

        @pl.when(need_s(other, l))
        def _():
            x_copy(c, l, q).start()

    lax.fori_loop(0, Q, encode, 0)
    for cp in lw:
        cp.wait()

    def decode_own(c):
        def own(q, carry):
            decode(c, l, q)
            return carry

        lax.fori_loop(0, Q, own, 0)

    def arrive(c, i):
        k = 1 + i // Q
        q = lax.rem(i, Q)

        def take(s, relay, on):
            blk = act_ref(c, s, q)
            rdma(blk, blk, x_s.at[c, s, q], z_r.at[c, s, q], xdev).wait_recv()

            @pl.when(on)
            def _():
                relay(c, s, q).start()

            @pl.when(need_s(other, s))
            def _():
                x_copy(c, s, q).start()

            decode(c, s, q)

        @pl.when(l - k >= 0)
        def _():
            take(l - k, z_right, has_r)

        @pl.when(l + k <= L - 1)
        def _():
            take(l + k, z_left, has_l)

    def arrivals(c, lo, hi):
        def step(i, carry):
            arrive(c, i)
            return carry

        if lo < hi:
            lax.fori_loop(lo, hi, step, 0)

    def derr_block(c, owner):
        return derr.at[:, brow(c * F + owner, B), :]

    def r1_copy(c, j):
        return rdma(r1b.at[c, j], r1r.at[c, j], r1_s.at[c, j], r1_r.at[c, j], sdev)

    def r2_wait(c, k):
        return rdma(r1r.at[c, 0], r2r.at[c, k - 1], r2_s.at[c, k], r2_r.at[c, k], sdev)

    def dx_copy(c, t):
        return rdma(derr.at[t, pl.ds(c * R, R), :], derr.at[t, pl.ds(n + c * R, R), :], dx_s.at[c, t], dx_r.at[c, t], xdev)

    def mid_pack(c):
        for k in range(1, H + 1):
            j = lax.rem(chip + k, H)
            rows = brow(2 * j + 1 - core, B)
            for t in range(L):
                r1b[c, j, t] = acc[c, t, rows, :].astype(BF)
            r1_copy(c, j).start()

    def mid_sum(c):
        for k in range(1, H):
            j, dev = peer(k)
            r1_copy(c, j).wait_recv()
            for t in range(L):
                r1r[c, j, t] = (acc[c, t, brow(dev, B), :] + r1r[c, j, t].astype(F32)).astype(BF)
            rdma(r1r.at[c, j], r2r.at[c, H - k - 1], r2_s.at[c, k], r2_r.at[c, H - k], (g, l, dev)).start()
        r1_copy(c, chip).wait_recv()
        for t in range(L):
            acc[c, t, brow(f, B), :] += (
                r1r[c, chip, t].astype(F32) + db[pl.ds(t, 1), :] - tgt[t, pl.ds(c * B, B), :].astype(F32)
            )

    def mid_err(c):
        for k in range(1, H):
            r2_wait(c, k).wait_recv()
        for t in range(L):
            err = acc[c, t, brow(f, B), :]
            for k in range(1, H):
                err = err + r2r[c, k - 1, t].astype(F32)
            acc[c, t, brow(f, B), :] = err
            derr[t, brow(c * F + f, B), :] = (err / total).astype(BF)
        mine = derr_block(c, f)
        for k in range(1, H):
            _, dev = peer(k)
            rdma(mine, mine, ag_p.at[c, k], ag_r.at[c, f], (g, l, dev)).start()
        rdma(mine, mine, ag_s.at[c, f], ag_r.at[c, f], sdev).start()
        for t in range(L):
            dbs[pl.ds(t, 1), :] += jnp.sum(acc[c, t, brow(f, B), :], axis=0, keepdims=True)

    def mid_relay(c):
        for k in range(1, H):
            _, dev = peer(k)
            blk = derr_block(c, dev)
            rdma(blk, blk, ag_p.at[c, k], ag_r.at[c, dev], sdev).wait_recv()
            rdma(blk, blk, ag_s.at[c, dev], ag_r.at[c, dev], sdev).start()

    def mid_end(c):
        for j in range(H):
            own = 2 * j + 1 - core
            blk = derr_block(c, own)
            rdma(blk, blk, ag_s.at[c, own], ag_r.at[c, own], sdev).wait_recv()
        for t in range(L):
            @pl.when(need_t(other, t))
            def _():
                dx_copy(c, t).start()

    def slot_ref(slot, c, q):
        return ew_v.at[q, brow(slot * C + c, R), :]

    def partial(c, s, q):
        acc[c, 0, :, pl.ds(0, cw)] = dot_nn(derr[s, pl.ds(c * R, R), :], w_v[pair(s, s), :, brow(q, cw)])

        def one(t, carry):
            acc[c, 0, :, pl.ds(0, cw)] += dot_nn(derr[t, pl.ds(c * R, R), :], w_v[pair(s, t), :, brow(q, cw)])
            return carry

        lax.fori_loop(s + 1, L, one, 0)

    def b_wait(slot, c, q):
        blk = slot_ref(slot, c, q)
        rdma(blk, blk, b_s.at[c, 0, q], b_r.at[c, slot, q], xdev).wait_recv()

    def b_right(c, s, q):
        return rdma(slot_ref(s, c, q), slot_ref(s, c, q), b_s.at[c, s, q], b_r.at[c, s, q], rdev)

    def b_left(c, s, q):
        to = jnp.where(s == l - 1, L, s)
        return rdma(slot_ref(s, c, q), slot_ref(to, c, q), b_s.at[c, s, q], b_r.at[c, to, q], ldev)

    order = [sorted(range(L), key=lambda s: (-abs(s - at), -s if at < L // 2 else s)) for at in range(L)]

    def source_at(k):
        s = jnp.int32(0)
        for at in range(L):
            for j in range(L - 1):
                s = jnp.where(jnp.logical_and(l == at, k == j), order[at][j], s)
        return s

    def send_job(c, i):
        s, q = source_at(i // Q), lax.rem(i, Q)
        partial(c, s, q)
        inner = jnp.where(s > l, has_l, has_r)

        @pl.when(inner)
        def _():
            b_wait(s, c, q)
            acc[c, 0, :, pl.ds(0, cw)] += slot_ref(s, c, q)[...].astype(F32)

        slot_ref(s, c, q)[...] = acc[c, 0, :, pl.ds(0, cw)].astype(BF)

        @pl.when(s > l)
        def _():
            b_right(c, s, q).start()

        @pl.when(s < l)
        def _():
            b_left(c, s, q).start()

    def dp_copy(c, q):
        return rdma(dpre.at[q, pl.ds(c * R, R), :], dpre.at[q, pl.ds(n + c * R, R), :], dp_s.at[c, q], dp_r.at[c, q], xdev)

    def own_job(c, q):
        partial(c, l, q)

        @pl.when(has_l)
        def _():
            b_wait(l, c, q)
            acc[c, 0, :, pl.ds(0, cw)] += slot_ref(l, c, q)[...].astype(F32)

        @pl.when(has_r)
        def _():
            b_wait(L, c, q)
            acc[c, 0, :, pl.ds(0, cw)] += slot_ref(L, c, q)[...].astype(F32)

        grad = jnp.where(act_ref(c, l, q)[...].astype(F32) > 0.0, acc[c, 0, :, pl.ds(0, cw)], 0.0)
        ebs[:, brow(q, cw)] += jnp.sum(grad, axis=0, keepdims=True)
        dpre[q, pl.ds(c * R, R), :] = grad.astype(BF)
        dp_copy(c, q).start()

    starts = [pair(s, s) for s in range(L)]

    def pair_of(p):
        s = jnp.int32(0)
        first = jnp.int32(0)
        for k in range(1, L):
            s = jnp.where(p >= starts[k], k, s)
            first = jnp.where(p >= starts[k], starts[k], first)
        return s, p - first + s

    def og_copy(i):
        slot, q = i // Q, lax.rem(i, Q)
        at = lax.rem(i, 2)
        return pltpu.make_async_copy(og_v.at[at], dg_o.at[slot, :, brow(q, cw)], og_m.at[at])

    def grad_job(i, carry):
        q = lax.rem(i, Q)
        s, t = pair_of(g * per + i // Q)

        @pl.when(i >= 2)
        def _():
            og_copy(i - 2).wait()

        if derr_t is None:
            grad = dot_tn(derr[t], acts[s, q])
        else:
            grad = dot_nn(derr_t[t], acts[s, q])
        og_v[lax.rem(i, 2)] = grad.astype(BF)
        og_copy(i).start()
        return carry

    def eg_copy(q):
        at = lax.rem(q, 2)
        return pltpu.make_async_copy(eg_v.at[at], eg_o.at[0, :, pl.ds(pl.multiple_of(q * cw, cw), cw)], eg_m.at[at])

    def enc_job(q):
        for c in range(C):
            dp_copy(c, q).wait_recv()

        @pl.when(q >= 2)
        def _():
            eg_copy(q - 2).wait()

        eg_v[lax.rem(q, 2)] = dot_nn(cols_t[...], dpre[q]).astype(BF)
        eg_copy(q).start()

    def turn_cols():
        cols = pl.ds(pl.multiple_of(g * half, half), half)
        cols_copy().wait_recv()
        cols_t[:, pl.ds(0, n)] = rows_v[:, cols].T
        cols_t[:, pl.ds(n, n)] = cols_o[...].T

    def wait_others():
        for c in range(C):
            for s in range(L):
                @pl.when(need_s(g, s))
                def _():
                    def one(q, carry):
                        x_copy(c, s, q).wait_recv()
                        return carry

                    lax.fori_loop(0, Q, one, 0)
            for t in range(L):
                @pl.when(need_t(g, t))
                def _():
                    dx_copy(c, t).wait_recv()
        if derr_t is not None:
            for t in range(L):
                @pl.when(need_t(g, t))
                def _():
                    derr_t[t] = derr[t].T

    jobs = per * Q
    steps = (L - 1) * Q

    def cut(i):
        return min(i, steps)

    def send_jobs(c, lo, hi):
        def step(i, carry):
            send_job(c, i)
            return carry

        if lo < hi:
            lax.fori_loop(lo, hi, step, 0)

    decode_own(0)
    arrivals(0, 0, cut(8))
    turn_cols()
    arrivals(0, cut(8), steps)

    def send_second(q, carry):
        send_own(1, q)
        return carry

    lax.fori_loop(0, Q, send_second, 0)
    mid_pack(0)
    mid_sum(0)
    decode_own(1)
    arrivals(1, 0, cut(1))
    mid_err(0)
    arrivals(1, cut(1), cut(4))
    mid_relay(0)
    arrivals(1, cut(4), cut(5))
    mid_end(0)

    def both(i, carry):
        send_job(0, i)
        arrive(1, i + cut(5))
        return carry

    lead = steps - cut(5)
    if lead > 0:
        lax.fori_loop(0, lead, both, 0)
    mid_pack(1)
    send_jobs(0, lead, cut(lead + 1))
    mid_sum(1)
    send_jobs(0, cut(lead + 1), cut(lead + 3))
    mid_err(1)
    for k in range(1, F):
        dev = lax.rem(f + k, F)
        rdma(dbs, dbr.at[F - k], db_s.at[k], db_r.at[F - k], (g, l, dev)).start()
    send_jobs(0, cut(lead + 3), steps)
    mid_relay(1)
    mid_end(1)

    def second(i, carry):
        send_job(1, i)

        @pl.when(jnp.logical_and(i >= 1, i < 1 + Q))
        def _():
            own_job(0, i - 1)

        base = 2 * (i - wait_at)

        @pl.when(i == wait_at)
        def _():
            wait_others()

        lax.fori_loop(jnp.minimum(jnp.maximum(base, 0), jobs), jnp.minimum(jnp.maximum(base + 2, 0), jobs), grad_job, 0)
        return carry

    wait_at = min(3, steps - 1)
    lax.fori_loop(0, steps, second, 0)
    for q in range(max(steps - 1, 0), Q):
        own_job(0, jnp.int32(q))
    lax.fori_loop(min(jobs, 2 * (steps - wait_at)), jobs, grad_job, 0)

    sums = dbs[...]
    for k in range(1, F):
        rdma(dbs, dbr.at[k], db_s.at[k], db_r.at[k], sdev).wait_recv()
        sums = sums + dbr[k]
    dbx[0] = sums
    dbx_copy = rdma(dbx.at[0], dbx.at[1], dbx_m.at[0], dbx_m.at[1], xdev)
    dbx_copy.start()

    def last(q, carry):
        own_job(1, q)

        @pl.when(q >= 1)
        def _():
            enc_job(q - 1)

        return carry

    lax.fori_loop(0, Q, last, 0)
    eb_copy = rdma(ebs, ebr, eb_m.at[0], eb_m.at[1], xdev)
    eb_copy.start()
    enc_job(jnp.int32(Q - 1))
    dbx_copy.wait()
    dbg_o[...] = (dbx[0] + dbx[1]) / total
    eb_copy.wait()
    ebg_o[...] = ebs[...] + ebr[...]

    cols_copy().wait_send()
    for i in range(max(0, jobs - 2), jobs):
        og_copy(jnp.int32(i)).wait()
    for q in range(max(0, Q - 2), Q):
        eg_copy(jnp.int32(q)).wait()
    for k in range(1, F):
        rdma(dbs, dbr.at[k], db_s.at[k], db_r.at[k], sdev).wait_send()
    for c in range(C):
        for k in range(1, H):
            mine = row_block(c, f)
            rdma(mine, mine, in_p.at[c, k], in_r.at[c, f], sdev).wait_send()
            r2_wait(c, k).wait_send()
            blk = derr_block(c, f)
            rdma(blk, blk, ag_p.at[c, k], ag_r.at[c, f], sdev).wait_send()
        for j in range(H):
            r1_copy(c, j).wait_send()
            own = 2 * j + core
            blk = row_block(c, own)
            rdma(blk, blk, in_s.at[c, own], in_r.at[c, own], sdev).wait_send()
            blk = derr_block(c, own)
            rdma(blk, blk, ag_s.at[c, own], ag_r.at[c, own], sdev).wait_send()
        for t in range(L):
            @pl.when(need_t(other, t))
            def _():
                dx_copy(c, t).wait_send()

        def drain(q, carry):
            for s in range(L):
                @pl.when(jnp.logical_and(has_r, s <= l))
                def _():
                    z_right(c, s, q).wait_send()

                @pl.when(jnp.logical_and(has_l, s >= l))
                def _():
                    z_left(c, s, q).wait_send()

                @pl.when(need_s(other, s))
                def _():
                    x_copy(c, s, q).wait_send()

                @pl.when(s != l)
                def _():
                    b_right(c, s, q).wait_send()
            dp_copy(c, q).wait_send()
            return carry

        lax.fori_loop(0, Q, drain, 0)


def per_device(chunks, inputs, targets, enc_weight, enc_bias, dec_weight, dec_bias):
    L = lax.axis_size("layer")
    F = lax.axis_size("feat")
    G = lax.axis_size("grp")
    assert G == 2 and F % 2 == 0
    pairs = pair_list(L)
    per = len(pairs) // G
    tok_dev, D = inputs.shape[1], inputs.shape[2]
    feats, width = dec_weight.shape[1], dec_weight.shape[2]
    C = chunks
    B = tok_dev // C
    R = F * B
    n = C * R
    H = F // 2
    total = tok_dev * F * G
    cw = min(512, feats // 2)
    Q = feats // cw
    groups = [pairs[h * per:(h + 1) * per] for h in range(G)]
    ranges = (
        tuple(min(s for s, _ in grp) for grp in groups),
        tuple(max(s for s, _ in grp) for grp in groups),
        tuple(min(t for _, t in grp) for grp in groups),
        tuple(max(t for _, t in grp) for grp in groups),
    )
    turned = n <= 512
    cfg = (L, F, C, B, D, feats, width, cw, per, total, ranges, turned)
    V = pltpu.VMEM
    S = pltpu.SemaphoreType.DMA
    slots = max(D, (L + 1) * n)
    scratch = [
        V((len(pairs), width, feats), BF), V((Q, slots, cw), BF), V((L, Q, 2 * n, cw), BF),
        V((n, D), BF), V((n, D // 2), BF), V((D // 2, 2 * n), BF), V((C, L, R, width), F32),
        V((L, 2 * n, width), BF), *([V((L, width, 2 * n), BF)] if turned else []),
        V((C, H, L, B, width), BF), V((C, H, L, B, width), BF), V((C, H - 1, L, B, width), BF),
        V((Q, 2 * n, cw), BF), V((2, width, cw), BF), V((min(2, Q), D // 2, cw), BF),
        V((L, width), F32), V((F, L, width), F32), V((2, L, width), F32), V((1, feats), F32), V((1, feats), F32),
        S((len(pairs),)), S((Q,)), S((C,)), S((C, H)), S((C, F)), S((C, F)), S((2,)),
        S((C, L, Q)), S((C, L, Q)), S((C, L, Q)), S((C, L, Q)), S((C, L, Q)), S((C, H)), S((C, H)), S((C, H)), S((C, H)),
        S((C, H)), S((C, F)), S((C, F)), S((C, L)), S((C, L)), S((F,)), S((F,)), S((2,)), S((2,)),
        S((C, L, Q)), S((C, L + 1, Q)), S((C, Q)), S((C, Q)), S((2,)), S((2,)),
    ]
    hbm = pl.BlockSpec(memory_space=pl.ANY)
    vm = pl.BlockSpec(memory_space=pltpu.VMEM)
    enc, encb, dec, decb = pl.pallas_call(
        functools.partial(kernel, cfg),
        out_shape=(
            jax.ShapeDtypeStruct((1, D // 2, feats), BF),
            jax.ShapeDtypeStruct((1, feats), F32),
            jax.ShapeDtypeStruct((per, width, feats), BF),
            jax.ShapeDtypeStruct((L, width), F32),
        ),
        in_specs=[hbm, vm, hbm, vm, hbm, vm],
        out_specs=(hbm, vm, hbm, vm),
        scratch_shapes=scratch,
        compiler_params=pltpu.CompilerParams(
            collective_id=0, has_side_effects=True, vmem_limit_bytes=67043328
        ),
        name="transcoder",
    )(inputs, jnp.swapaxes(targets, 0, 1), enc_weight, enc_bias, jnp.swapaxes(dec_weight, 1, 2), dec_bias)
    return enc, encb, jnp.swapaxes(dec, 1, 2), decb


def solution(mesh):
    return jax.shard_map(
        functools.partial(per_device, CHUNKS),
        mesh=mesh,
        in_specs=(
            P("layer", ("grp", "feat"), None),
            P(("grp", "feat"), None, "layer"),
            P("layer", None, "feat"),
            P("layer", "feat"),
            P(None, "feat", "layer"),
            P(None, "layer"),
        ),
        out_specs=(
            P("layer", "grp", "feat"),
            P("layer", "feat"),
            P("grp", "feat", "layer"),
            P(None, "layer"),
        ),
        check_vma=False,
    )
```

```python
import functools

import jax
import jax.numpy as jnp
from jax import lax
from jax.experimental import pallas as pl
from jax.experimental.pallas import tpu as pltpu
from jax.sharding import PartitionSpec as P

MESH = pl.DeviceIdType.MESH
BF = jnp.bfloat16
F32 = jnp.float32


def pair_list(count):
    return [(source, target) for source in range(count) for target in range(source, count)]


CHUNKS = 2


def dot_nn(a, b):
    return lax.dot_general(a, b, (((1,), (0,)), ((), ())), preferred_element_type=F32)


def dot_nt(a, b):
    return lax.dot_general(a, b, (((1,), (1,)), ((), ())), preferred_element_type=F32)


def dot_tn(a, b):
    return lax.dot_general(a, b, (((0,), (0,)), ((), ())), preferred_element_type=F32)


def rdma(src, dst, ssem, rsem, dev):
    return pltpu.make_async_remote_copy(
        src_ref=src, dst_ref=dst, send_sem=ssem, recv_sem=rsem, device_id=dev, device_id_type=MESH
    )


def kernel(cfg, *refs):
    (L, F, C, B, D, feats, width, cw, per, total, ranges, turned) = cfg
    if not turned:
        refs = refs[:18] + (None,) + refs[18:]
    (inp, tgt, ew, eb, dw, db, eg_o, ebg_o, dg_o, dbg_o,
     w_v, ew_v, acts, rows_v, cols_o, cols_t, acc, derr, derr_t,
     r1b, r1r, r2r, dpre, og_v, eg_v, dbs, dbr, dbx, ebs, ebr,
     ld_w, ld_ew, ld_in, in_p, in_s, in_r, co, zr_s, zl_s, z_r, x_s, x_r, r1_s, r1_r, r2_s, r2_r,
     ag_p, ag_s, ag_r, dx_s, dx_r, db_s, db_r, dbx_m, eb_m, b_s, b_r, dp_s, dp_r, og_m, eg_m) = refs
    g = lax.axis_index("grp")
    l = lax.axis_index("layer")
    f = lax.axis_index("feat")
    Q = feats // cw
    R = F * B
    n = C * R
    H = F // 2
    half = D // 2
    core = lax.rem(f, 2)
    chip = f // 2
    sib = f + 1 - 2 * core
    other = 1 - g
    xdev, sdev = (other, l, f), (g, l, sib)
    rdev, ldev = (g, l + 1, f), (g, l - 1, f)
    has_l, has_r = l > 0, l < L - 1

    def peer(k):
        j = lax.rem(chip + k, H)
        return j, 2 * j + core

    def by_group(which, values):
        return jnp.where(which == 0, values[0], values[1])

    def pair(s, t):
        return s * L - (s * (s - 1)) // 2 + t - s

    def brow(idx, n):
        return pl.ds(pl.multiple_of(idx * n, n), n)

    def need_s(h, s):
        return jnp.logical_and(s >= by_group(h, ranges[0]), s <= by_group(h, ranges[1]))

    def need_t(h, t):
        return jnp.logical_and(t >= by_group(h, ranges[2]), t <= by_group(h, ranges[3]))

    lin = [pltpu.make_async_copy(inp.at[0, pl.ds(c * B, B), :], rows_v.at[brow(c * F + f, B), :], ld_in.at[c])
           for c in range(C)]
    for cp in lin:
        cp.start()
    lew = [pltpu.make_async_copy(ew.at[0, :, pl.ds(q * cw, cw)], ew_v.at[q, pl.ds(0, D), :], ld_ew.at[q])
           for q in range(Q)]
    for cp in lew:
        cp.start()
    lw = [pltpu.make_async_copy(dw.at[p], w_v.at[p], ld_w.at[p]) for p in range(2 * per)]
    for cp in lw:
        cp.start()

    bar = pltpu.get_barrier_semaphore()
    pl.semaphore_signal(bar, inc=1, device_id=xdev, device_id_type=MESH)
    for k in range(1, F):
        pl.semaphore_signal(bar, inc=1, device_id=(g, l, lax.rem(f + k, F)), device_id_type=MESH)

    @pl.when(has_l)
    def _():
        pl.semaphore_signal(bar, inc=1, device_id=ldev, device_id_type=MESH)

    @pl.when(has_r)
    def _():
        pl.semaphore_signal(bar, inc=1, device_id=rdev, device_id_type=MESH)

    pl.semaphore_wait(bar, F + has_l.astype(jnp.int32) + has_r.astype(jnp.int32))

    def row_block(c, owner):
        return rows_v.at[brow(c * F + owner, B), :]

    for c in range(C):
        lin[c].wait()
        mine = row_block(c, f)
        for k in range(1, H):
            _, dev = peer(k)
            rdma(mine, mine, in_p.at[c, k], in_r.at[c, f], (g, l, dev)).start()
        rdma(mine, mine, in_s.at[c, f], in_r.at[c, f], sdev).start()
    def rows_ready(c):
        for k in range(1, H):
            _, dev = peer(k)
            blk = row_block(c, dev)
            rdma(blk, blk, in_p.at[c, k], in_r.at[c, dev], sdev).wait_recv()
            rdma(blk, blk, in_s.at[c, dev], in_r.at[c, dev], sdev).start()
        for j in range(H):
            own = 2 * j + 1 - core
            blk = row_block(c, own)
            rdma(blk, blk, in_s.at[c, own], in_r.at[c, own], sdev).wait_recv()

    dbs[...] = jnp.zeros_like(dbs)
    ebs[...] = jnp.zeros_like(ebs)
    acc[0] = jnp.zeros(acc.shape[1:], F32)
    rows_ready(0)

    def cols_copy():
        cols = pl.ds(pl.multiple_of(other * half, half), half)
        return rdma(rows_v.at[:, cols], cols_o, co.at[0], co.at[1], xdev)

    def act_ref(c, s, q):
        return acts.at[s, q, pl.ds(c * R, R), :]

    def z_right(c, s, q):
        blk = act_ref(c, s, q)
        return rdma(blk, blk, zr_s.at[c, s, q], z_r.at[c, s, q], rdev)

    def z_left(c, s, q):
        blk = act_ref(c, s, q)
        return rdma(blk, blk, zl_s.at[c, s, q], z_r.at[c, s, q], ldev)

    def x_copy(c, s, q):
        return rdma(act_ref(c, s, q), acts.at[s, q, pl.ds(n + c * R, R), :], x_s.at[c, s, q], x_r.at[c, s, q], xdev)

    def decode(c, s, q):
        def one(t, carry):
            acc[c, t] += dot_nt(act_ref(c, s, q)[...], w_v[pair(s, t), :, brow(q, cw)])
            return carry

        lax.fori_loop(s, L, one, 0)

    def encode(c, count, q):
        bias = eb[:, pl.ds(pl.multiple_of(q * cw, cw), cw)]
        pre = dot_nn(rows_v[pl.ds(c * R, count * R), :], ew_v[q, pl.ds(0, D), :]) + bias
        acts[l, q, pl.ds(c * R, count * R), :] = jnp.maximum(pre, 0.0).astype(BF)

    def weights_ready(q):
        pltpu.make_async_copy(
            ew.at[0, :, pl.ds(pl.multiple_of(q * cw, cw), cw)], ew_v.at[q, pl.ds(0, D), :], ld_ew.at[q]
        ).wait()

    def send_own(c, q):
        @pl.when(has_r)
        def _():
            z_right(c, l, q).start()

        @pl.when(has_l)
        def _():
            z_left(c, l, q).start()

        @pl.when(need_s(other, l))
        def _():
            x_copy(c, l, q).start()

    def encode_first(q, carry):
        weights_ready(q)
        encode(0, 1, q)
        send_own(0, q)
        return carry

    def encode_second(q, carry):
        encode(1, 1, q)
        return carry

    lax.fori_loop(0, Q - 1, encode_first, 0)
    rows_ready(1)
    cols_copy().start()
    lax.fori_loop(0, Q - 1, encode_second, 0)
    weights_ready(jnp.int32(Q - 1))
    encode(0, 2, jnp.int32(Q - 1))
    send_own(0, jnp.int32(Q - 1))
    acc[1] = jnp.zeros(acc.shape[1:], F32)
    for cp in lw:
        cp.wait()

    def decode_own(c):
        def own(q, carry):
            decode(c, l, q)
            return carry

        lax.fori_loop(0, Q, own, 0)

    def arrive(c, i):
        k = 1 + i // Q
        q = lax.rem(i, Q)

        def take(s, relay, on):
            blk = act_ref(c, s, q)
            rdma(blk, blk, x_s.at[c, s, q], z_r.at[c, s, q], xdev).wait_recv()

            @pl.when(on)
            def _():
                relay(c, s, q).start()

            @pl.when(need_s(other, s))
            def _():
                x_copy(c, s, q).start()

            decode(c, s, q)

        @pl.when(l - k >= 0)
        def _():
            take(l - k, z_right, has_r)

        @pl.when(l + k <= L - 1)
        def _():
            take(l + k, z_left, has_l)

    def arrivals(c, lo, hi):
        def step(i, carry):
            arrive(c, i)
            return carry

        if lo < hi:
            lax.fori_loop(lo, hi, step, 0)

    def derr_block(c, owner):
        return derr.at[:, brow(c * F + owner, B), :]

    def r1_copy(c, j):
        return rdma(r1b.at[c, j], r1r.at[c, j], r1_s.at[c, j], r1_r.at[c, j], sdev)

    def r2_wait(c, k):
        return rdma(r1r.at[c, 0], r2r.at[c, k - 1], r2_s.at[c, k], r2_r.at[c, k], sdev)

    def dx_copy(c, t):
        return rdma(derr.at[t, pl.ds(c * R, R), :], derr.at[t, pl.ds(n + c * R, R), :], dx_s.at[c, t], dx_r.at[c, t], xdev)

    def mid_pack(c):
        for k in range(1, H + 1):
            j = lax.rem(chip + k, H)
            rows = brow(2 * j + 1 - core, B)
            for t in range(L):
                r1b[c, j, t] = acc[c, t, rows, :].astype(BF)
            r1_copy(c, j).start()

    def mid_sum(c):
        for k in range(1, H):
            j, dev = peer(k)
            r1_copy(c, j).wait_recv()
            for t in range(L):
                r1r[c, j, t] = (acc[c, t, brow(dev, B), :] + r1r[c, j, t].astype(F32)).astype(BF)
            rdma(r1r.at[c, j], r2r.at[c, H - k - 1], r2_s.at[c, k], r2_r.at[c, H - k], (g, l, dev)).start()
        r1_copy(c, chip).wait_recv()
        for t in range(L):
            acc[c, t, brow(f, B), :] += (
                r1r[c, chip, t].astype(F32) + db[pl.ds(t, 1), :] - tgt[pl.ds(c * B, B), t, :].astype(F32)
            )

    def mid_err(c):
        for k in range(1, H):
            r2_wait(c, k).wait_recv()
        for t in range(L):
            err = acc[c, t, brow(f, B), :]
            for k in range(1, H):
                err = err + r2r[c, k - 1, t].astype(F32)
            acc[c, t, brow(f, B), :] = err
            derr[t, brow(c * F + f, B), :] = (err / total).astype(BF)
        mine = derr_block(c, f)
        for k in range(1, H):
            _, dev = peer(k)
            rdma(mine, mine, ag_p.at[c, k], ag_r.at[c, f], (g, l, dev)).start()
        rdma(mine, mine, ag_s.at[c, f], ag_r.at[c, f], sdev).start()
        for t in range(L):
            dbs[pl.ds(t, 1), :] += jnp.sum(acc[c, t, brow(f, B), :], axis=0, keepdims=True)

    def mid_relay(c):
        for k in range(1, H):
            _, dev = peer(k)
            blk = derr_block(c, dev)
            rdma(blk, blk, ag_p.at[c, k], ag_r.at[c, dev], sdev).wait_recv()
            rdma(blk, blk, ag_s.at[c, dev], ag_r.at[c, dev], sdev).start()

    def mid_end(c):
        for j in range(H):
            own = 2 * j + 1 - core
            blk = derr_block(c, own)
            rdma(blk, blk, ag_s.at[c, own], ag_r.at[c, own], sdev).wait_recv()
        for t in range(L):
            @pl.when(need_t(other, t))
            def _():
                dx_copy(c, t).start()

    def slot_ref(slot, c, q):
        return ew_v.at[q, brow(slot * C + c, R), :]

    def partial(c, s, q):
        acc[c, 0, :, pl.ds(0, cw)] = dot_nn(derr[s, pl.ds(c * R, R), :], w_v[pair(s, s), :, brow(q, cw)])

        def one(t, carry):
            acc[c, 0, :, pl.ds(0, cw)] += dot_nn(derr[t, pl.ds(c * R, R), :], w_v[pair(s, t), :, brow(q, cw)])
            return carry

        lax.fori_loop(s + 1, L, one, 0)

    def b_wait(slot, c, q):
        blk = slot_ref(slot, c, q)
        rdma(blk, blk, b_s.at[c, 0, q], b_r.at[c, slot, q], xdev).wait_recv()

    def b_right(c, s, q):
        return rdma(slot_ref(s, c, q), slot_ref(s, c, q), b_s.at[c, s, q], b_r.at[c, s, q], rdev)

    def b_left(c, s, q):
        to = jnp.where(s == l - 1, L, s)
        return rdma(slot_ref(s, c, q), slot_ref(to, c, q), b_s.at[c, s, q], b_r.at[c, to, q], ldev)

    order = [sorted(range(L), key=lambda s: (-abs(s - at), -s if at < L // 2 else s)) for at in range(L)]

    def source_at(k):
        s = jnp.int32(0)
        for at in range(L):
            for j in range(L - 1):
                s = jnp.where(jnp.logical_and(l == at, k == j), order[at][j], s)
        return s

    def send_job(c, i):
        s, q = source_at(i // Q), lax.rem(i, Q)
        partial(c, s, q)
        inner = jnp.where(s > l, has_l, has_r)

        @pl.when(inner)
        def _():
            b_wait(s, c, q)
            acc[c, 0, :, pl.ds(0, cw)] += slot_ref(s, c, q)[...].astype(F32)

        slot_ref(s, c, q)[...] = acc[c, 0, :, pl.ds(0, cw)].astype(BF)

        @pl.when(s > l)
        def _():
            b_right(c, s, q).start()

        @pl.when(s < l)
        def _():
            b_left(c, s, q).start()

    def dp_copy(c, q):
        return rdma(dpre.at[q, pl.ds(c * R, R), :], dpre.at[q, pl.ds(n + c * R, R), :], dp_s.at[c, q], dp_r.at[c, q], xdev)

    def own_job(c, q):
        partial(c, l, q)

        @pl.when(has_l)
        def _():
            b_wait(l, c, q)
            acc[c, 0, :, pl.ds(0, cw)] += slot_ref(l, c, q)[...].astype(F32)

        @pl.when(has_r)
        def _():
            b_wait(L, c, q)
            acc[c, 0, :, pl.ds(0, cw)] += slot_ref(L, c, q)[...].astype(F32)

        grad = jnp.where(act_ref(c, l, q)[...].astype(F32) > 0.0, acc[c, 0, :, pl.ds(0, cw)], 0.0)
        ebs[:, brow(q, cw)] += jnp.sum(grad, axis=0, keepdims=True)
        dpre[q, pl.ds(c * R, R), :] = grad.astype(BF)
        dp_copy(c, q).start()

    starts = [pair(s, s) for s in range(L)]

    def pair_of(p):
        s = jnp.int32(0)
        first = jnp.int32(0)
        for k in range(1, L):
            s = jnp.where(p >= starts[k], k, s)
            first = jnp.where(p >= starts[k], starts[k], first)
        return s, p - first + s

    def og_copy(i):
        slot, q = i // Q, lax.rem(i, Q)
        at = lax.rem(i, 2)
        return pltpu.make_async_copy(og_v.at[at], dg_o.at[slot, :, brow(q, cw)], og_m.at[at])

    def grad_job(i, carry):
        q = lax.rem(i, Q)
        s, t = pair_of(g * per + i // Q)

        @pl.when(i >= 2)
        def _():
            og_copy(i - 2).wait()

        if derr_t is None:
            grad = dot_tn(derr[t], acts[s, q])
        else:
            grad = dot_nn(derr_t[t], acts[s, q])
        og_v[lax.rem(i, 2)] = grad.astype(BF)
        og_copy(i).start()
        return carry

    def eg_copy(q):
        at = lax.rem(q, 2)
        return pltpu.make_async_copy(eg_v.at[at], eg_o.at[0, :, pl.ds(pl.multiple_of(q * cw, cw), cw)], eg_m.at[at])

    def enc_job(q):
        for c in range(C):
            dp_copy(c, q).wait_recv()

        @pl.when(q >= 2)
        def _():
            eg_copy(q - 2).wait()

        eg_v[lax.rem(q, 2)] = dot_nn(cols_t[...], dpre[q]).astype(BF)
        eg_copy(q).start()

    def turn_cols():
        cols = pl.ds(pl.multiple_of(g * half, half), half)
        cols_copy().wait_recv()
        cols_t[:, pl.ds(0, n)] = rows_v[:, cols].T
        cols_t[:, pl.ds(n, n)] = cols_o[...].T

    def wait_others():
        for c in range(C):
            for s in range(L):
                @pl.when(need_s(g, s))
                def _():
                    def one(q, carry):
                        x_copy(c, s, q).wait_recv()
                        return carry

                    lax.fori_loop(0, Q, one, 0)
            for t in range(L):
                @pl.when(need_t(g, t))
                def _():
                    dx_copy(c, t).wait_recv()
        if derr_t is not None:
            for t in range(L):
                @pl.when(need_t(g, t))
                def _():
                    derr_t[t] = derr[t].T

    jobs = per * Q
    steps = (L - 1) * Q

    def cut(i):
        return min(i, steps)

    def send_jobs(c, lo, hi):
        def step(i, carry):
            send_job(c, i)
            return carry

        if lo < hi:
            lax.fori_loop(lo, hi, step, 0)

    decode_own(0)
    arrivals(0, 0, cut(8))
    turn_cols()
    arrivals(0, cut(8), steps)

    def send_second(q, carry):
        send_own(1, q)
        return carry

    lax.fori_loop(0, Q, send_second, 0)
    mid_pack(0)
    mid_sum(0)
    decode_own(1)
    arrivals(1, 0, cut(1))
    mid_err(0)
    arrivals(1, cut(1), cut(4))
    mid_relay(0)
    arrivals(1, cut(4), cut(5))
    mid_end(0)

    def both(i, carry):
        send_job(0, i)
        arrive(1, i + cut(5))
        return carry

    lead = steps - cut(5)
    if lead > 0:
        lax.fori_loop(0, lead, both, 0)
    mid_pack(1)
    send_jobs(0, lead, cut(lead + 1))
    mid_sum(1)
    send_jobs(0, cut(lead + 1), cut(lead + 2))
    mid_err(1)
    for k in range(1, F):
        dev = lax.rem(f + k, F)
        rdma(dbs, dbr.at[F - k], db_s.at[k], db_r.at[F - k], (g, l, dev)).start()
    send_jobs(0, cut(lead + 2), cut(lead + 4))
    mid_relay(1)
    send_jobs(0, cut(lead + 4), steps)
    mid_end(1)

    ahead = jnp.where(jnp.logical_and(has_l, has_r), 0, steps)

    def early(i, carry):
        send_job(1, i)
        return carry

    lax.fori_loop(0, ahead, early, 0)

    def second(i, carry):
        @pl.when(i >= ahead)
        def _():
            send_job(1, i)

        @pl.when(jnp.logical_and(i >= 1, i < 1 + Q))
        def _():
            own_job(0, i - 1)

        base = 3 * (i - wait_at)

        @pl.when(i == wait_at)
        def _():
            wait_others()

        lax.fori_loop(jnp.minimum(jnp.maximum(base, 0), jobs), jnp.minimum(jnp.maximum(base + 3, 0), jobs), grad_job, 0)
        return carry

    wait_at = min(5, steps - 1)
    lax.fori_loop(0, steps, second, 0)
    for q in range(max(steps - 1, 0), Q):
        own_job(0, jnp.int32(q))
    lax.fori_loop(min(jobs, 3 * (steps - wait_at)), jobs, grad_job, 0)

    sums = dbs[...]
    for k in range(1, F):
        rdma(dbs, dbr.at[k], db_s.at[k], db_r.at[k], sdev).wait_recv()
        sums = sums + dbr[k]
    dbx[0] = sums
    dbx_copy = rdma(dbx.at[0], dbx.at[1], dbx_m.at[0], dbx_m.at[1], xdev)
    dbx_copy.start()

    def last(q, carry):
        own_job(1, q)

        @pl.when(q >= 1)
        def _():
            enc_job(q - 1)

        return carry

    lax.fori_loop(0, Q, last, 0)
    eb_copy = rdma(ebs, ebr, eb_m.at[0], eb_m.at[1], xdev)
    eb_copy.start()
    enc_job(jnp.int32(Q - 1))
    dbx_copy.wait()
    dbg_o[...] = (dbx[0] + dbx[1]) / total
    eb_copy.wait()
    ebg_o[...] = ebs[...] + ebr[...]

    cols_copy().wait_send()
    for i in range(max(0, jobs - 2), jobs):
        og_copy(jnp.int32(i)).wait()
    for q in range(max(0, Q - 2), Q):
        eg_copy(jnp.int32(q)).wait()
    for k in range(1, F):
        rdma(dbs, dbr.at[k], db_s.at[k], db_r.at[k], sdev).wait_send()
    for c in range(C):
        for k in range(1, H):
            mine = row_block(c, f)
            rdma(mine, mine, in_p.at[c, k], in_r.at[c, f], sdev).wait_send()
            r2_wait(c, k).wait_send()
            blk = derr_block(c, f)
            rdma(blk, blk, ag_p.at[c, k], ag_r.at[c, f], sdev).wait_send()
        for j in range(H):
            r1_copy(c, j).wait_send()
            own = 2 * j + core
            blk = row_block(c, own)
            rdma(blk, blk, in_s.at[c, own], in_r.at[c, own], sdev).wait_send()
            blk = derr_block(c, own)
            rdma(blk, blk, ag_s.at[c, own], ag_r.at[c, own], sdev).wait_send()
        for t in range(L):
            @pl.when(need_t(other, t))
            def _():
                dx_copy(c, t).wait_send()

        def drain(q, carry):
            for s in range(L):
                @pl.when(jnp.logical_and(has_r, s <= l))
                def _():
                    z_right(c, s, q).wait_send()

                @pl.when(jnp.logical_and(has_l, s >= l))
                def _():
                    z_left(c, s, q).wait_send()

                @pl.when(need_s(other, s))
                def _():
                    x_copy(c, s, q).wait_send()

                @pl.when(s != l)
                def _():
                    b_right(c, s, q).wait_send()
            dp_copy(c, q).wait_send()
            return carry

        lax.fori_loop(0, Q, drain, 0)


def per_device(chunks, inputs, targets, enc_weight, enc_bias, dec_weight, dec_bias):
    L = lax.axis_size("layer")
    F = lax.axis_size("feat")
    G = lax.axis_size("grp")
    assert G == 2 and F % 2 == 0
    pairs = pair_list(L)
    per = len(pairs) // G
    tok_dev, D = inputs.shape[1], inputs.shape[2]
    feats, width = dec_weight.shape[1], dec_weight.shape[2]
    C = chunks
    B = tok_dev // C
    R = F * B
    n = C * R
    H = F // 2
    total = tok_dev * F * G
    cw = min(512, feats // 2)
    Q = feats // cw
    groups = [pairs[h * per:(h + 1) * per] for h in range(G)]
    ranges = (
        tuple(min(s for s, _ in grp) for grp in groups),
        tuple(max(s for s, _ in grp) for grp in groups),
        tuple(min(t for _, t in grp) for grp in groups),
        tuple(max(t for _, t in grp) for grp in groups),
    )
    turned = n <= 512
    cfg = (L, F, C, B, D, feats, width, cw, per, total, ranges, turned)
    V = pltpu.VMEM
    S = pltpu.SemaphoreType.DMA
    slots = max(D, (L + 1) * n)
    scratch = [
        V((len(pairs), width, feats), BF), V((Q, slots, cw), BF), V((L, Q, 2 * n, cw), BF),
        V((n, D), BF), V((n, D // 2), BF), V((D // 2, 2 * n), BF), V((C, L, R, width), F32),
        V((L, 2 * n, width), BF), *([V((L, width, 2 * n), BF)] if turned else []),
        V((C, H, L, B, width), BF), V((C, H, L, B, width), BF), V((C, H - 1, L, B, width), BF),
        V((Q, 2 * n, cw), BF), V((2, width, cw), BF), V((min(2, Q), D // 2, cw), BF),
        V((L, width), F32), V((F, L, width), F32), V((2, L, width), F32), V((1, feats), F32), V((1, feats), F32),
        S((len(pairs),)), S((Q,)), S((C,)), S((C, H)), S((C, F)), S((C, F)), S((2,)),
        S((C, L, Q)), S((C, L, Q)), S((C, L, Q)), S((C, L, Q)), S((C, L, Q)), S((C, H)), S((C, H)), S((C, H)), S((C, H)),
        S((C, H)), S((C, F)), S((C, F)), S((C, L)), S((C, L)), S((F,)), S((F,)), S((2,)), S((2,)),
        S((C, L, Q)), S((C, L + 1, Q)), S((C, Q)), S((C, Q)), S((2,)), S((2,)),
    ]
    hbm = pl.BlockSpec(memory_space=pl.ANY)
    vm = pl.BlockSpec(memory_space=pltpu.VMEM)
    enc, encb, dec, decb = pl.pallas_call(
        functools.partial(kernel, cfg),
        out_shape=(
            jax.ShapeDtypeStruct((1, D // 2, feats), BF),
            jax.ShapeDtypeStruct((1, feats), F32),
            jax.ShapeDtypeStruct((per, width, feats), BF),
            jax.ShapeDtypeStruct((L, width), F32),
        ),
        in_specs=[hbm, vm, hbm, vm, hbm, vm],
        out_specs=(hbm, vm, hbm, vm),
        scratch_shapes=scratch,
        compiler_params=pltpu.CompilerParams(
            collective_id=0, has_side_effects=True, vmem_limit_bytes=67043328
        ),
        name="transcoder",
    )(inputs, targets, enc_weight, enc_bias, jnp.swapaxes(dec_weight, 1, 2), dec_bias)
    parts, wide = 2, 8

    def hand_on(enc_ref, dec_ref, enc_out, dec_out):
        enc_out[...] = enc_ref[...]
        dec_out[...] = dec_ref[...]

    dec_spec = pl.BlockSpec((1, width // parts, feats), lambda i: (i // parts, i % parts, 0))
    enc_spec = pl.BlockSpec((1, D // 2 // wide, feats), lambda i: (0, jnp.minimum(i, wide - 1), 0))
    assert per * parts >= wide
    enc, dec = pl.pallas_call(
        hand_on,
        grid=(per * parts,),
        out_shape=(jax.ShapeDtypeStruct(enc.shape, BF), jax.ShapeDtypeStruct(dec.shape, BF)),
        in_specs=[enc_spec, dec_spec],
        out_specs=(enc_spec, dec_spec),
        name="hand_on",
    )(enc, dec)
    return enc, encb, jnp.swapaxes(dec, 1, 2), decb


def solution(mesh):
    return jax.shard_map(
        functools.partial(per_device, CHUNKS),
        mesh=mesh,
        in_specs=(
            P("layer", ("grp", "feat"), None),
            P(("grp", "feat"), None, "layer"),
            P("layer", None, "feat"),
            P("layer", "feat"),
            P(None, "feat", "layer"),
            P(None, "layer"),
        ),
        out_specs=(
            P("layer", "grp", "feat"),
            P("layer", "feat"),
            P("grp", "feat", "layer"),
            P(None, "layer"),
        ),
        check_vma=False,
    )
```
